32 devices in a mesh: gx: 2 (over core), gy: 2 (over y), gz: 8 (over z, x).
Axes of the slice: x: 2, y: 2, z: 4, core: 2. Of those that a mesh axis runs over, the one named last changes fastest.
Arguments:
- right_side: float32 [8192, 2048], P(('gx', 'gy'), 'gz'), may hold values from -6 to 6
- send_order: int32 [4, 2048], P(('gx', 'gy')), may hold values from 0 to 2047, each once within a row
- recv_order: int32 [4, 2048], P(('gx', 'gy')), may hold values from 0 to 2047, each once within a row
- update_target: int32 [16, 2], P('gx'), may hold values from 0 to 15, as said below
- leaf_inv: float32 [16, 256, 256], P(('gx', 'gy'), 'gz'), may hold values from -0.375 to 0.375
- leaf_low: float32 [16, 256, 256], P(('gx', 'gy'), 'gz'), may hold values from -0.375 to 0.375
- parent_inv: float32 [8, 512, 512], P(('gx', 'gy'), 'gz'), may hold values from -0.25 to 0.25
Outputs:
- solution: float32 [8192, 2048], P(('gx', 'gy'), 'gz')
The draws below stay inside these ranges and needn't reach their ends.
Inputs may be any that keep to these rules, and one draw needn't show every extreme that they name: `update_target`: entries are 4 * parent + block, with parent counted among the 2 * 2 parents of the leaf's gx index and block below 4; a leaf's two entries name the same parent and two different blocks. Among the 4 leaves of one index of gx+gy, at most 2 name parents held by one index of gy (parent // 2), and exactly 2 do so for some index of gy.
All inputs are finite; a program needn't handle non-finite values.
Results may differ from the reference program's by a relative error of at most 0.000073.
Values sent between devices are 32-bit elements; how exact they have to be, the bound alone decides.
No kernel may reach another device: no remote copies, remote signals or barrier semaphores. Data moves between devices by JAX's collectives and lax.ppermute only.
A program may use at most 64 MiB of HBM per device.

```python
import jax
import jax.numpy as jnp
from jax import lax

PIV = 256
BLK = 128
LEAF_DEV = 4
PAR_DEV = 2
NXY = 4
ROWS_DEV = 2048
ORDER = 8192
RHS = 2048
LEAVES = 16
PARENTS = 8
N_GX = 2
N_GY = 2


def draw_update_target(key, part):
    base = jax.random.fold_in(key, 11)
    key_one, key_two, key_three, key_four = jax.random.split(base, 4)
    groups = N_GX * N_GY
    perm_keys = jax.random.split(key_one, groups)
    orders = jax.vmap(lambda single: jax.random.permutation(single, N_GY))(perm_keys).astype(jnp.int32)
    positions = jnp.arange(LEAF_DEV, dtype=jnp.int32) % N_GY
    owners = orders[:, positions]
    within = jax.random.randint(key_two, (groups, LEAF_DEV), 0, PAR_DEV).astype(jnp.int32)
    parent = (owners * PAR_DEV + within).reshape(-1)
    total = LEAF_DEV * groups
    first = jax.random.randint(key_three, (total,), 0, 4).astype(jnp.int32)
    stride = jax.random.randint(key_four, (total,), 1, 4).astype(jnp.int32)
    second = (first + stride) % 4
    return jnp.stack([parent * 4 + first, parent * 4 + second], axis=1).astype(jnp.int32)


def block_scale(key, dims, pieces, smallest, largest):
    gain = 1.0
    for position, parts in pieces:
        steps = jax.random.uniform(jax.random.fold_in(jax.random.fold_in(key, 6), position), (parts,), jnp.float32, smallest / len(pieces), largest / len(pieces))
        gain = gain * jnp.repeat(jnp.exp(steps), dims[position] // parts).reshape((-1,) + (1,) * (len(dims) - 1 - position))
    return gain


def bell_draw(own_key, extent, width, limit, shards=(), held_as=jnp.bfloat16):
    values = jax.random.normal(own_key, extent, jnp.float32) * width
    if len(shards) > 0:
        values = block_scale(own_key, extent, shards, -0.22, 0.18) * values
    return jnp.clip(values, min=-limit, max=limit).astype(held_as)


def setup_inputs(seed: int = 0) -> dict:
    key_of = jax.random.split(jax.random.key(seed), 8)
    return {
        "right_side": bell_draw(key_of[0], (ORDER, RHS), 1.0, 6.0, ((0, 4), (1, 8)), jnp.float32),
        "send_order": jax.vmap(lambda own: jax.random.permutation(own, ROWS_DEV))(jax.random.split(key_of[1], NXY)).reshape((NXY, ROWS_DEV)).astype(jnp.int32),
        "recv_order": jax.vmap(lambda own: jax.random.permutation(own, ROWS_DEV))(jax.random.split(key_of[2], NXY)).reshape((NXY, ROWS_DEV)).astype(jnp.int32),
        "update_target": draw_update_target(jax.random.fold_in(key_of[7], 71), 0),
        "leaf_inv": bell_draw(key_of[4], (LEAVES, PIV, PIV), PIV ** -0.5, 0.375, ((0, 4), (1, 8)), jnp.float32),
        "leaf_low": bell_draw(key_of[5], (LEAVES, 2 * BLK, PIV), PIV ** -0.5, 0.375, ((0, 4), (1, 8)), jnp.float32),
        "parent_inv": bell_draw(key_of[6], (PARENTS, 4 * BLK, 4 * BLK), (4 * BLK) ** -0.5, 0.25, ((0, 4), (1, 8)), jnp.float32),
    }


def reference(right_side, send_order, recv_order, update_target, leaf_inv, leaf_low, parent_inv):
    nxy = N_GX * N_GY
    count = ROWS_DEV // nxy
    base = jnp.arange(nxy, dtype=jnp.int32)[:, None] * ROWS_DEV + send_order.astype(jnp.int32)
    routed = base.reshape(nxy, nxy, count).transpose(1, 0, 2).reshape(nxy, ROWS_DEV)
    picked = jnp.take_along_axis(routed, recv_order.astype(jnp.int32), axis=1).reshape(-1)
    front = right_side[picked].reshape(nxy, ROWS_DEV, RHS)
    leaf_rhs = front[:, :LEAF_DEV * PIV].reshape(LEAVES, PIV, RHS)
    parent_rhs = front[:, LEAF_DEV * PIV:].reshape(PARENTS, 4 * BLK, RHS)
    leaf_sol = jnp.einsum("fij,fjc->fic", leaf_inv, leaf_rhs, precision=lax.Precision.HIGHEST)
    update = jnp.einsum("fij,fjc->fic", leaf_low, leaf_sol, precision=lax.Precision.HIGHEST)
    group = jnp.arange(LEAVES, dtype=jnp.int32) // (LEAF_DEV * N_GY)
    targets = (group[:, None] * (PAR_DEV * N_GY * 4) + update_target.astype(jnp.int32)).reshape(-1)
    contribution = jax.ops.segment_sum(update.reshape(LEAVES * 2, BLK, RHS), targets, num_segments=PARENTS * 4)
    contribution = contribution.reshape(PARENTS, 4 * BLK, RHS)
    parent_sol = jnp.einsum("pij,pjc->pic", parent_inv, parent_rhs - contribution, precision=lax.Precision.HIGHEST)
    joined = jnp.concatenate([leaf_sol.reshape(nxy, LEAF_DEV * PIV, RHS), parent_sol.reshape(nxy, PAR_DEV * 4 * BLK, RHS)], axis=1)
    return joined.reshape(ORDER, RHS)
```

```python
import functools

import jax
import jax.numpy as jnp
from jax import lax
from jax.experimental import pallas as pl
from jax.experimental.pallas import tpu as pltpu
from jax.sharding import PartitionSpec as P

PIV = 256
BLK = 128
LEAF_DEV = 4
PAR_DEV = 2
OWN_BLOCKS = PAR_DEV * 4
LEAF_ROWS = LEAF_DEV * PIV
PAR_ROWS = PAR_DEV * 4 * BLK


SMEM = pltpu.SMEM
VMEM = pltpu.VMEM


def cost(flops, size):
    return pl.CostEstimate(flops=flops, bytes_accessed=size, transcendentals=0)


def split(value):
    high = value.astype(jnp.bfloat16)
    low = (value - high.astype(jnp.float32)).astype(jnp.bfloat16)
    return high, low


def product(a_high, a_low, b):
    b_high, b_low = split(b)
    dot = functools.partial(jnp.dot, preferred_element_type=jnp.float32)
    return dot(a_high, b_high) + (dot(a_high, b_low) + dot(a_low, b_high))


def copy_rows(order_ref, start, source, target, target_start, count, unroll=16):
    def step(j, carry):
        base = j * unroll
        for u in range(unroll):
            row = order_ref[start + base + u]
            target[pl.ds(target_start + base + u, 1), :] = source[pl.ds(row, 1), :]
        return carry

    lax.fori_loop(0, count // unroll, step, 0)


def pack_kernel(relatives, count, index_ref, order_ref, rows_ref, *out_refs):
    own = index_ref[0]
    for relative, out_ref in zip(relatives, out_refs):
        copy_rows(order_ref, (own ^ relative) * count, rows_ref, out_ref, 0, count)


def pack(index, order, right_side, relatives, count, chunk, width):
    rows = right_side.shape[0]
    return pl.pallas_call(
        functools.partial(pack_kernel, relatives, count),
        grid=(1,),
        out_shape=[jax.ShapeDtypeStruct((count, width), jnp.float32)] * len(relatives),
        in_specs=[
            pl.BlockSpec(memory_space=SMEM),
            pl.BlockSpec(memory_space=SMEM),
            pl.BlockSpec((rows, width), lambda i: (0, chunk)),
        ],
        out_specs=[pl.BlockSpec((count, width), lambda i: (0, 0))] * len(relatives),
        cost_estimate=cost(40_000_000, 4 * rows * width),
        name="pack",
    )(index, order, right_side)


def order_kernel(pieces, order_ref, *refs):
    piece_refs, out_ref, arrived, sems = refs[:pieces], refs[pieces], refs[pieces + 1], refs[pieces + 2]
    rows = out_ref.shape[0]
    each = rows // pieces
    copies = [
        pltpu.make_async_copy(ref, arrived.at[pl.ds(k * each, each), :], sems.at[k])
        for k, ref in enumerate(piece_refs)
    ]
    for copy in copies:
        copy.start()
    for copy in copies:
        copy.wait()
    copy_rows(order_ref, 0, arrived, out_ref, 0, rows)


def order_rows(order, pieces):
    rows = sum(piece.shape[0] for piece in pieces)
    width = pieces[0].shape[1]
    return pl.pallas_call(
        functools.partial(order_kernel, len(pieces)),
        out_shape=jax.ShapeDtypeStruct((rows, width), jnp.float32),
        in_specs=[pl.BlockSpec(memory_space=SMEM)] + [pl.BlockSpec(memory_space=pltpu.HBM)] * len(pieces),
        out_specs=pl.BlockSpec(memory_space=VMEM),
        scratch_shapes=[VMEM((rows, width), jnp.float32), pltpu.SemaphoreType.DMA((len(pieces),))],
        cost_estimate=cost(60_000_000, 8 * rows * width),
        name="order",
    )(order, *pieces)


def ring_order(n):
    return list(range(0, n, 2)) + list(range(n - 1 - n % 2, 0, -2))


def ring_gather(block, axis):
    n = lax.axis_size(axis)
    ring = ring_order(n)
    forward = [(ring[i], ring[(i + 1) % n]) for i in range(n)]
    backward = [(b, a) for a, b in forward]
    pieces = [(block, 0, 0)]
    ahead = behind = block
    for step in range(1, (n - 1) // 2 + 1):
        ahead = lax.ppermute(ahead, axis, forward)
        behind = lax.ppermute(behind, axis, backward)
        pieces += [(ahead, 0, step), (behind, 0, -step)]
    if n % 2 == 0 and n > 1:
        half = block.shape[0] // 2
        pieces.append((lax.ppermute(ahead[:half], axis, forward), 0, n // 2))
        pieces.append((lax.ppermute(behind[half:], axis, backward), half, n // 2))
    return pieces


def piece_places(axis, pieces):
    n = lax.axis_size(axis)
    ring = jnp.array(ring_order(n), jnp.int32)
    at = jnp.argsort(ring)[lax.axis_index(axis)]
    steps = jnp.array([steps for _, _, steps in pieces], jnp.int32)
    return ring[(at - steps) % n].astype(jnp.int32)


def assemble(place_ref, refs, firsts, high, low):
    for k, (ref, first) in enumerate(zip(refs, firsts)):
        count, rows, _ = ref.shape
        at = pl.ds(pl.multiple_of(place_ref[k] * rows, rows), rows)
        for i in range(count):
            h, l = split(ref[i])
            high[first + i, at, :] = h
            low[first + i, at, :] = l


def owner_and_rank(target_ref, first_row):
    owners = [target_ref[first_row + l, 0] // (4 * PAR_DEV) for l in range(LEAF_DEV)]
    ranks = []
    for l in range(LEAF_DEV):
        rank = jnp.int32(0)
        for m in range(l):
            rank = rank + (owners[m] == owners[l]).astype(jnp.int32)
        ranks.append(rank)
    return owners, ranks


def leaf_kernel(firsts, capacity, groups, gy_ref, target_ref, place_ref, *refs):
    pieces = len(firsts)
    rhs_ref = refs[0]
    inv_refs, low_refs = refs[1 : 1 + pieces], refs[1 + pieces : 1 + 2 * pieces]
    refs = refs[1 + 2 * pieces :]
    if len(refs) == 1 + groups + 6:
        refs = refs[1:]
    out_ref, slot_refs = refs[0], refs[1 : 1 + groups]
    inv_high, inv_low, low_high, low_low, update = refs[1 + groups :]
    assemble(place_ref, inv_refs, firsts, inv_high, inv_low)
    assemble(place_ref, low_refs, firsts, low_high, low_low)
    for l in range(LEAF_DEV):
        rows = pl.ds(l * PIV, PIV)
        sol = product(inv_high[l], inv_low[l], rhs_ref[rows, :])
        out_ref[rows, :] = sol
        update[l] = product(low_high[l], low_low[l], sol)
    own = gy_ref[0]
    owners, ranks = owner_and_rank(target_ref, own * LEAF_DEV)
    for k in range(groups):
        for r in range(capacity):
            chosen = jnp.int32(0)
            for l in range(LEAF_DEV):
                chosen = jnp.where((owners[l] == (own ^ k)) & (ranks[l] == r), l, chosen)
            slot_refs[k][r] = update[chosen]


def solve_leaves(gy, target, places, front, inv_pieces, low_pieces, partial, chunk, columns, capacity, groups):
    width = front.shape[1]
    firsts = [first for _, first, _ in inv_pieces]
    smem = pl.BlockSpec(memory_space=SMEM)
    whole = [pl.BlockSpec(p.shape, lambda i: (0, 0, 0)) for p, _, _ in inv_pieces + low_pieces]
    slot = (capacity, 2 * BLK, width)
    matrix = VMEM((LEAF_DEV, PIV, PIV), jnp.bfloat16)
    return pl.pallas_call(
        functools.partial(leaf_kernel, firsts, capacity, groups),
        grid=(1,),
        out_shape=[jax.ShapeDtypeStruct((front.shape[0], columns), jnp.float32)]
        + [jax.ShapeDtypeStruct(slot, jnp.float32)] * groups,
        in_specs=[smem, smem, smem, pl.BlockSpec((LEAF_ROWS, width), lambda i: (0, 0))]
        + whole
        + ([pl.BlockSpec(memory_space=pl.ANY)] if partial is not None else []),
        out_specs=[pl.BlockSpec((LEAF_ROWS, width), lambda i: (0, chunk))]
        + [pl.BlockSpec(slot, lambda i: (0, 0, 0))] * groups,
        scratch_shapes=[matrix] * 4 + [VMEM((LEAF_DEV, 2 * BLK, width), jnp.float32)],
        input_output_aliases={4 + len(whole): 0} if partial is not None else {},
        cost_estimate=cost(100_000_000, 4 << 20),
        name="leaves",
    )(
        gy,
        target,
        places,
        front,
        *[p for p, _, _ in inv_pieces],
        *[p for p, _, _ in low_pieces],
        *([partial] if partial is not None else []),
    )


def parent_kernel(firsts, groups, gy_ref, target_ref, place_ref, rhs_ref, *refs):
    pieces = len(firsts)
    slot_refs, inv_refs = refs[:groups], refs[groups : groups + pieces]
    out_ref, inv_high, inv_low, reduced = refs[groups + pieces + 1 :]
    assemble(place_ref, inv_refs, firsts, inv_high, inv_low)
    own = gy_ref[0]
    reduced[...] = rhs_ref[...]
    for k in range(groups):
        first_row = (own ^ k) * LEAF_DEV
        owners, ranks = owner_and_rank(target_ref, first_row)
        for l in range(LEAF_DEV):

            @pl.when(owners[l] == own)
            def _():
                for j in range(2):
                    block = target_ref[first_row + l, j] % OWN_BLOCKS
                    at = pl.ds(pl.multiple_of(block * BLK, BLK), BLK)
                    reduced[at, :] = reduced[at, :] - slot_refs[k][ranks[l], pl.ds(j * BLK, BLK), :]

    size = 4 * BLK
    for p in range(PAR_DEV):
        rows = pl.ds(p * size, size)
        out_ref[rows, :] = product(inv_high[p], inv_low[p], reduced[rows, :])


def solve_parents(gy, target, places, front, slots, inv_pieces, partial, chunk):
    width = front.shape[1]
    firsts = [first for _, first, _ in inv_pieces]
    smem = pl.BlockSpec(memory_space=SMEM)
    zeros = lambda i: (0, 0, 0)
    matrix = VMEM((PAR_DEV, 4 * BLK, 4 * BLK), jnp.bfloat16)
    return pl.pallas_call(
        functools.partial(parent_kernel, firsts, len(slots)),
        grid=(1,),
        out_shape=jax.ShapeDtypeStruct(partial.shape, jnp.float32),
        in_specs=[smem, smem, smem, pl.BlockSpec((PAR_ROWS, width), lambda i: (1, 0))]
        + [pl.BlockSpec(s.shape, zeros) for s in slots]
        + [pl.BlockSpec(p.shape, zeros) for p, _, _ in inv_pieces]
        + [pl.BlockSpec(memory_space=pl.ANY)],
        out_specs=pl.BlockSpec((PAR_ROWS, width), lambda i: (1, chunk)),
        scratch_shapes=[matrix] * 2 + [VMEM((PAR_ROWS, width), jnp.float32)],
        input_output_aliases={4 + len(slots) + len(inv_pieces): 0},
        cost_estimate=cost(100_000_000, 4 << 20),
        name="parents",
    )(gy, target, places, front, *slots, *[p for p, _, _ in inv_pieces], partial)


def body(chunks, right_side, send_order, recv_order, update_target, leaf_inv, leaf_low, parent_inv):
    columns = right_side.shape[1]
    width = columns // chunks
    both = ("gx", "gy")
    n = lax.axis_size(both)
    groups = lax.axis_size("gy")
    rows = right_side.shape[0]
    count = rows // n
    own = (lax.axis_index("gx") * groups + lax.axis_index("gy")).astype(jnp.int32)
    index = own.reshape(1)
    gy = lax.axis_index("gy").astype(jnp.int32).reshape(1)
    target = update_target.astype(jnp.int32)
    send = send_order[0]
    capacity = (LEAF_DEV + groups - 1) // groups

    inv_pieces = ring_gather(leaf_inv, "gz")
    low_pieces = ring_gather(leaf_low, "gz")
    parent_pieces = ring_gather(parent_inv, "gz")
    places = piece_places("gz", inv_pieces)

    direct = n <= 8
    arrived = []
    for c in range(chunks):
        if direct:
            far = [k for k in range(n) if k % groups]
            near = [k for k in range(n) if k % groups == 0]
            packed = dict(zip(far, pack(index, send, right_side, far, count, c, width)))
            packed.update(zip(near, pack(index, send, right_side, near, count, c, width)))
            arrived.append(
                [
                    lax.ppermute(packed[k], both, [(e, e ^ k) for e in range(n)]) if k else packed[0]
                    for k in range(n)
                ]
            )
        else:
            outgoing = jnp.take(right_side[:, c * width : (c + 1) * width], send, axis=0, mode="clip")
            arrived.append([lax.all_to_all(outgoing, both, split_axis=0, concat_axis=0, tiled=True)])
    recv = recv_order[0]
    if direct:
        recv = ((recv // count) ^ own) * count + recv % count
    fronts = [order_rows(recv, pieces) for pieces in arrived]

    out = None
    slots = []
    for c in range(chunks):
        out, *local = solve_leaves(
            gy, target, places, fronts[c], inv_pieces, low_pieces, out, c, columns, capacity, groups
        )
        slots.append(
            [lax.ppermute(s, "gy", [(g, g ^ k) for g in range(groups)]) if k else s for k, s in enumerate(local)]
        )
    for c in range(chunks):
        out = solve_parents(gy, target, places, fronts[c], slots[c], parent_pieces, out, c)
    return out


def solution(mesh):
    placed = (
        P(("gx", "gy"), "gz"),
        P(("gx", "gy"), None),
        P(("gx", "gy"), None),
        P("gx", None),
        P(("gx", "gy"), "gz", None),
        P(("gx", "gy"), "gz", None),
        P(("gx", "gy"), "gz", None),
    )
    return jax.shard_map(
        functools.partial(body, 1), mesh=mesh, in_specs=placed, out_specs=P(("gx", "gy"), "gz"), check_vma=False
    )
```

```python
import functools

import jax
import jax.numpy as jnp
from jax import lax
from jax.experimental import pallas as pl
from jax.experimental.pallas import tpu as pltpu
from jax.sharding import PartitionSpec as P

PIV = 256
BLK = 128
LEAF_DEV = 4
PAR_DEV = 2
LANES = 128
SUBLANES = 8
OWN_BLOCKS = PAR_DEV * 4
LEAF_ROWS = LEAF_DEV * PIV
PAR_ROWS = PAR_DEV * 4 * BLK


SMEM = pl.BlockSpec(memory_space=pltpu.SMEM)
VMEM = pl.BlockSpec(memory_space=pltpu.VMEM)


def call(kernel, name, flops, grant, out_shape, in_specs, out_specs, scratch_shapes=()):
    return pl.pallas_call(
        kernel,
        out_shape=out_shape,
        in_specs=in_specs,
        out_specs=out_specs,
        scratch_shapes=scratch_shapes,
        cost_estimate=pl.CostEstimate(flops=flops, bytes_accessed=2 << 20, transcendentals=0),
        compiler_params=pltpu.CompilerParams(vmem_limit_bytes=grant << 20),
        name=name,
    )


def split(value):
    high = value.astype(jnp.bfloat16)
    low = (value - high.astype(jnp.float32)).astype(jnp.bfloat16)
    return high, low


def product(a_high, a_low, b):
    b_high, b_low = split(b)
    dot = functools.partial(jnp.dot, preferred_element_type=jnp.float32)
    return dot(a_high, b_high) + (dot(a_high, b_low) + dot(a_low, b_high))


def to_tiles(rows):
    r, c = rows.shape
    tiles = rows.reshape(r // SUBLANES, SUBLANES, c // LANES, LANES).transpose(0, 2, 1, 3)
    return tiles.reshape(r * (c // LANES), LANES)


def copy_rows(order_ref, start, source, target, count, strips, unroll=16):
    def step(j, carry):
        base = pl.multiple_of(j * unroll, unroll)
        for u in range(unroll):
            row = order_ref[0, start + base + u]
            at = row * strips - (row & (SUBLANES - 1)) * (strips - 1)
            to = (u // SUBLANES) * SUBLANES * strips + u % SUBLANES
            value = source[pl.ds(at, strips, stride=SUBLANES), :]
            target[pl.ds(base * strips + to, strips, stride=SUBLANES), :] = value
        return carry

    lax.fori_loop(0, count // unroll, step, 0)


def index_of(axes):
    index = jnp.int32(0)
    for axis in axes:
        index = index * lax.axis_size(axis) + lax.axis_index(axis)
    return index


def pack_kernel(relatives, count, strips, order_ref, rows_ref, *out_refs):
    own = index_of(("gx", "gy"))
    for relative, out_ref in zip(relatives, out_refs):
        copy_rows(order_ref, (own ^ relative) * count, rows_ref, out_ref, count, strips)


def pack(order, tiles, relatives, count, strips):
    shape = jax.ShapeDtypeStruct((count * strips, LANES), jnp.float32)
    return call(
        functools.partial(pack_kernel, relatives, count, strips),
        "pack",
        10_000_000,
        8,
        [shape] * len(relatives),
        [SMEM, VMEM],
        [VMEM] * len(relatives),
    )(order, tiles)


def stack_arrived(piece_refs, arrived):
    own = index_of(("gx", "gy"))
    each = piece_refs[0].shape[0]
    for k, ref in enumerate(piece_refs):
        at = (own ^ k) * each if len(piece_refs) > 1 else 0
        arrived[pl.ds(pl.multiple_of(at, SUBLANES), each), :] = ref[...]


def strip_rows(ref, first, rows, strips):
    tiles = ref[pl.ds(first * strips, rows * strips), :].reshape(rows // SUBLANES, strips, SUBLANES, LANES)
    return jnp.concatenate([tiles[:, s].reshape(rows, LANES) for s in range(strips)], axis=1)


def ring_order(n):
    return list(range(0, n, 2)) + list(range(n - 1, 0, -2))


def ring_gather(block, axis, last_forward):
    n = lax.axis_size(axis)
    assert n % 2 == 0
    ring = ring_order(n)
    forward = [(ring[i], ring[(i + 1) % n]) for i in range(n)]
    backward = [(b, a) for a, b in forward]
    pieces = [(0, block)]
    ahead = behind = block
    for step in range(1, n // 2):
        ahead = lax.ppermute(ahead, axis, forward)
        behind = lax.ppermute(behind, axis, backward)
        pieces += [(step, ahead), (-step, behind)]
    last = lax.ppermute(ahead, axis, forward) if last_forward else lax.ppermute(behind, axis, backward)
    return pieces + [(n // 2, last)]


def place_of(steps):
    n = lax.axis_size("gz")
    index = lax.axis_index("gz")
    at = jnp.where(index % 2 == 0, index // 2, n - 1 - index // 2)
    to = (at - steps + n) % n
    return jnp.where(to < n // 2, 2 * to, 2 * (n - to) - 1)


def assemble(steps, refs, first, high, low):
    for step, ref in zip(steps, refs):
        count, rows, _ = ref.shape
        at = pl.ds(pl.multiple_of(place_of(step) * rows, rows), rows)
        for i in range(count):
            h, l = split(ref[i])
            high[first + i, at, :] = h
            low[first + i, at, :] = l


def owner_and_rank(target_ref, first_row):
    owners = [target_ref[0, first_row + l] // (4 * PAR_DEV) for l in range(LEAF_DEV)]
    ranks = []
    for l in range(LEAF_DEV):
        rank = jnp.int32(0)
        for m in range(l):
            rank = rank + (owners[m] == owners[l]).astype(jnp.int32)
        ranks.append(rank)
    return owners, ranks


def leaf_kernel(pieces, steps, capacity, groups, strips, order_ref, target_ref, *refs):
    piece_refs, refs = refs[:pieces], refs[pieces:]
    inv_refs, low_refs, refs = refs[: len(steps)], refs[len(steps) : 2 * len(steps)], refs[2 * len(steps) :]
    sol_ref, slot_refs = refs[0], refs[1 : 1 + groups]
    arrived, front, inv_high, inv_low, low_high, low_low, update = refs[1 + groups :]
    assemble(steps, inv_refs, 0, inv_high, inv_low)
    assemble(steps, low_refs, 0, low_high, low_low)
    stack_arrived(piece_refs, arrived)
    copy_rows(order_ref, 0, arrived, front, LEAF_ROWS, strips)
    for l in range(LEAF_DEV):
        sol = product(inv_high[l], inv_low[l], strip_rows(front, l * PIV, PIV, strips))
        sol_ref[pl.ds(l * PIV, PIV), :] = sol
        update[l] = product(low_high[l], low_low[l], sol)
    own = lax.axis_index("gy")
    owners, ranks = owner_and_rank(target_ref, own * LEAF_DEV)
    for k in range(groups):
        for r in range(capacity):
            chosen = jnp.int32(0)
            for l in range(LEAF_DEV):
                chosen = jnp.where((owners[l] == (own ^ k)) & (ranks[l] == r), l, chosen)
            slot_refs[k][r] = update[chosen]


def solve_leaves(order, target, pieces, inv_pieces, low_pieces, capacity, groups, strips):
    steps = [step for step, _ in inv_pieces]
    assert steps[:-1] == [step for step, _ in low_pieces][:-1]
    columns = strips * LANES
    slot = jax.ShapeDtypeStruct((capacity, 2 * BLK, columns), jnp.float32)
    matrix = pltpu.VMEM((LEAF_DEV, PIV, PIV), jnp.bfloat16)
    arrived = sum(piece.shape[0] for piece in pieces)
    return call(
        functools.partial(leaf_kernel, len(pieces), steps, capacity, groups, strips),
        "leaves",
        30_000_000,
        20,
        [jax.ShapeDtypeStruct((LEAF_ROWS, columns), jnp.float32)] + [slot] * groups,
        [SMEM, SMEM] + [VMEM] * (len(pieces) + 2 * len(steps)),
        [VMEM] * (1 + groups),
        [pltpu.VMEM((arrived, LANES), jnp.float32), pltpu.VMEM((LEAF_ROWS * strips, LANES), jnp.float32)]
        + [matrix] * 4
        + [pltpu.VMEM((LEAF_DEV, 2 * BLK, columns), jnp.float32)],
    )(order, target, *pieces, *[p for _, p in inv_pieces], *[p for _, p in low_pieces])


def gather_kernel(pieces, strips, order_ref, *refs):
    piece_refs, out_ref, arrived, front = refs[:pieces], *refs[pieces:]
    stack_arrived(piece_refs, arrived)
    copy_rows(order_ref, LEAF_ROWS, arrived, front, PAR_ROWS, strips)
    out_ref[...] = strip_rows(front, 0, PAR_ROWS, strips)


def gather_parents(order, pieces, strips):
    arrived = sum(piece.shape[0] for piece in pieces)
    return call(
        functools.partial(gather_kernel, len(pieces), strips),
        "parent_rows",
        10_000_000,
        12,
        jax.ShapeDtypeStruct((PAR_ROWS, strips * LANES), jnp.float32),
        [SMEM] + [VMEM] * len(pieces),
        VMEM,
        [pltpu.VMEM((arrived, LANES), jnp.float32), pltpu.VMEM((PAR_ROWS * strips, LANES), jnp.float32)],
    )(order, *pieces)


def parent_kernel(steps, groups, target_ref, sol_ref, rhs_ref, *refs):
    slot_refs, refs = refs[:groups], refs[groups:]
    inv_refs = [refs[p * len(steps) : (p + 1) * len(steps)] for p in range(PAR_DEV)]
    out_ref, inv_high, inv_low, reduced = refs[PAR_DEV * len(steps) :]
    for p in range(PAR_DEV):
        assemble(steps, inv_refs[p], p, inv_high, inv_low)
    own = lax.axis_index("gy")
    reduced[...] = rhs_ref[...]
    for k in range(groups):
        first_row = (own ^ k) * LEAF_DEV
        owners, ranks = owner_and_rank(target_ref, first_row)
        for l in range(LEAF_DEV):

            @pl.when(owners[l] == own)
            def _():
                for j in range(2):
                    block = target_ref[j, first_row + l] % OWN_BLOCKS
                    at = pl.ds(pl.multiple_of(block * BLK, BLK), BLK)
                    reduced[at, :] = reduced[at, :] - slot_refs[k][ranks[l], pl.ds(j * BLK, BLK), :]

    out_ref[pl.ds(0, LEAF_ROWS), :] = sol_ref[...]
    size = 4 * BLK
    for p in range(PAR_DEV):
        value = product(inv_high[p], inv_low[p], reduced[pl.ds(p * size, size), :])
        out_ref[pl.ds(LEAF_ROWS + p * size, size), :] = value


def solve_parents(target, sol, rhs, slots, inv_pieces):
    steps = [step for step, _ in inv_pieces[0]]
    columns = sol.shape[1]
    matrix = pltpu.VMEM((PAR_DEV, 4 * BLK, 4 * BLK), jnp.bfloat16)
    return call(
        functools.partial(parent_kernel, steps, len(slots)),
        "parents",
        30_000_000,
        20,
        jax.ShapeDtypeStruct((LEAF_ROWS + PAR_ROWS, columns), jnp.float32),
        [SMEM] + [VMEM] * (2 + len(slots) + PAR_DEV * len(steps)),
        VMEM,
        [matrix] * 2 + [pltpu.VMEM((PAR_ROWS, columns), jnp.float32)],
    )(target, sol, rhs, *slots, *[p for pieces in inv_pieces for _, p in pieces])


def body(right_side, send_order, recv_order, update_target, leaf_inv, leaf_low, parent_inv):
    both = ("gx", "gy")
    n = lax.axis_size(both)
    groups = lax.axis_size("gy")
    rows, columns = right_side.shape
    count = rows // n
    strips = columns // LANES
    capacity = (LEAF_DEV + groups - 1) // groups
    target = update_target.T

    inv_pieces = ring_gather(leaf_inv, "gz", True)
    low_pieces = ring_gather(leaf_low, "gz", False)
    parent_pieces = [ring_gather(parent_inv[p : p + 1], "gz", p % 2 == 0) for p in range(PAR_DEV)]

    if n <= 8:
        tiles = to_tiles(right_side)
        far = [k for k in range(n) if k % groups]
        near = [k for k in range(n) if k % groups == 0]
        packed = dict(zip(far, pack(send_order, tiles, far, count, strips)))
        packed.update(zip(near, pack(send_order, tiles, near, count, strips)))
        arrived = [
            lax.ppermute(packed[k], both, [(e, e ^ k) for e in range(n)]) if k else packed[0] for k in range(n)
        ]
    else:
        outgoing = jnp.take(right_side, send_order[0], axis=0, mode="clip")
        arrived = [to_tiles(lax.all_to_all(outgoing, both, split_axis=0, concat_axis=0, tiled=True))]

    sol, *slots = solve_leaves(recv_order, target, arrived, inv_pieces, low_pieces, capacity, groups, strips)
    parent_rhs = gather_parents(recv_order, arrived, strips)
    slots = [lax.ppermute(s, "gy", [(g, g ^ k) for g in range(groups)]) if k else s for k, s in enumerate(slots)]
    return solve_parents(target, sol, parent_rhs, slots, parent_pieces)


def solution(mesh):
    placed = (
        P(("gx", "gy"), "gz"),
        P(("gx", "gy"), None),
        P(("gx", "gy"), None),
        P("gx", None),
        P(("gx", "gy"), "gz", None),
        P(("gx", "gy"), "gz", None),
        P(("gx", "gy"), "gz", None),
    )
    return jax.shard_map(body, mesh=mesh, in_specs=placed, out_specs=P(("gx", "gy"), "gz"), check_vma=False)
```

```python
import functools

import jax
import jax.numpy as jnp
from jax import lax
from jax.experimental import pallas as pl
from jax.experimental.pallas import tpu as pltpu
from jax.sharding import PartitionSpec as P


PIV = 256
BLK = 128
LEAF_DEV = 4
PAR_DEV = 2
LANES = 128
SUBLANES = 8
OWN_BLOCKS = PAR_DEV * 4
LEAF_ROWS = LEAF_DEV * PIV
PAR_ROWS = PAR_DEV * 4 * BLK


SMEM = pl.BlockSpec(memory_space=pltpu.SMEM)
VMEM = pl.BlockSpec(memory_space=pltpu.VMEM)


def call(kernel, flops, grant, out_shape, in_specs, out_specs, scratch_shapes=()):
    return pl.pallas_call(
        kernel,
        out_shape=out_shape,
        in_specs=in_specs,
        out_specs=out_specs,
        scratch_shapes=scratch_shapes,
        cost_estimate=pl.CostEstimate(flops=flops, bytes_accessed=2 << 20, transcendentals=0),
        compiler_params=pltpu.CompilerParams(vmem_limit_bytes=int(grant * (1 << 20))),
    )


def split(value):
    high = value.astype(jnp.bfloat16)
    low = (value - high.astype(jnp.float32)).astype(jnp.bfloat16)
    return high, low


def product(a_high, a_low, b):
    b_high, b_low = split(b)
    dot = functools.partial(jnp.dot, preferred_element_type=jnp.float32)
    return dot(a_high, b_high) + (dot(a_high, b_low) + dot(a_low, b_high))


def to_tiles(rows):
    r, c = rows.shape
    tiles = rows.reshape(r // SUBLANES, SUBLANES, c // LANES, LANES).transpose(0, 2, 1, 3)
    return tiles.reshape(r * (c // LANES), LANES)


def tile_address(row, strips):
    return row * strips - (row & (SUBLANES - 1)) * (strips - 1)


def copy_rows(address_ref, start, source, target, count, strips, unroll=16):
    def step(j, carry):
        base = pl.multiple_of(j * unroll, unroll)
        for u in range(unroll):
            value = source[pl.ds(address_ref[0, start + base + u], strips, stride=SUBLANES), :]
            to = (u // SUBLANES) * SUBLANES * strips + u % SUBLANES
            target[pl.ds(base * strips + to, strips, stride=SUBLANES), :] = value
        return carry

    lax.fori_loop(0, count // unroll, step, 0)


def index_of(axes):
    index = jnp.int32(0)
    for axis in axes:
        index = index * lax.axis_size(axis) + lax.axis_index(axis)
    return index


def pack_kernel(relatives, count, strips, address_ref, rows_ref, *out_refs):
    own = index_of(("gx", "gy"))
    for relative, out_ref in zip(relatives, out_refs):
        copy_rows(address_ref, (own ^ relative) * count, rows_ref, out_ref, count, strips)


def pack(address, tiles, relatives, count, strips):
    shape = jax.ShapeDtypeStruct((count * strips, LANES), jnp.float32)
    return call(
        functools.partial(pack_kernel, relatives, count, strips),
        10_000_000,
        8,
        [shape] * len(relatives),
        [SMEM, VMEM],
        [VMEM] * len(relatives),
    )(address, tiles)


def stack_arrived(piece_refs, arrived):
    own = index_of(("gx", "gy"))
    each = piece_refs[0].shape[0]
    for k, ref in enumerate(piece_refs):
        at = (own ^ k) * each if len(piece_refs) > 1 else 0
        arrived[pl.ds(pl.multiple_of(at, SUBLANES), each), :] = ref[...]


def strip_rows(ref, first, rows, strips):
    at = pl.ds(pl.multiple_of(first * strips, SUBLANES), rows * strips)
    tiles = ref[at, :].reshape(rows // SUBLANES, strips, SUBLANES, LANES)
    return jnp.concatenate([tiles[:, s].reshape(rows, LANES) for s in range(strips)], axis=1)


def order_kernel(pieces, strips, address_ref, *refs):
    piece_refs, front_ref, arrived = refs[:pieces], *refs[pieces:]
    stack_arrived(piece_refs, arrived)
    copy_rows(address_ref, 0, arrived, front_ref, arrived.shape[0] // strips, strips)


def order_rows(address, pieces, strips):
    shape = (sum(piece.shape[0] for piece in pieces), LANES)
    return call(
        functools.partial(order_kernel, len(pieces), strips),
        10_000_000,
        12,
        jax.ShapeDtypeStruct(shape, jnp.float32),
        [SMEM] + [VMEM] * len(pieces),
        VMEM,
        [pltpu.VMEM(shape, jnp.float32)],
    )(address, *pieces)


def side_by_side(a, b):
    least = jnp.float32(-jnp.inf)
    rest = [(0, 0, 0)] * (a.ndim - 1)
    return jnp.maximum(
        lax.pad(a, least, [(0, b.shape[0], 0)] + rest), lax.pad(b, least, [(a.shape[0], 0, 0)] + rest)
    )


def ring_order(n):
    return list(range(0, n, 2)) + list(range(n - 1, 0, -2))


def ring_gather(block, axis):
    n = lax.axis_size(axis)
    assert n % 2 == 0
    ring = ring_order(n)
    forward = [(ring[i], ring[(i + 1) % n]) for i in range(n)]
    backward = [(b, a) for a, b in forward]

    def hop(value, way):
        return lax.ppermute(value, axis, forward if way == "f" else backward)

    pieces = [(0, block)]
    ahead = behind = block
    for step in range(1, n // 2):
        ahead, behind = hop(ahead, "f"), hop(behind, "b")
        pieces += [(step, ahead), (-step, behind)]
    half = block.shape[0] // 2
    return pieces, (hop(ahead[:half], "f"), hop(behind[half:], "b"))


def unzip(factors):
    pieces, halves = factors
    return [step for step, _ in pieces], [block for _, block in pieces] + list(halves)


def place_of(steps):
    n = lax.axis_size("gz")
    index = lax.axis_index("gz")
    at = jnp.where(index % 2 == 0, index // 2, n - 1 - index // 2)
    to = (at - steps + n) % n
    return jnp.where(to < n // 2, 2 * to, 2 * (n - to) - 1)


def assemble(steps, refs, entry, high, low):
    at_piece, half, at_half, slot = entry
    parts = [(step, ref, at_piece) for step, ref in zip(steps, refs)]
    parts.append((lax.axis_size("gz") // 2, refs[len(steps) + half], at_half))
    for step, ref, index in parts:
        rows = ref.shape[1]
        at = pl.ds(pl.multiple_of(place_of(step) * rows, rows), rows)
        high[slot, at, :], low[slot, at, :] = split(ref[index])


def owner_and_rank(target_ref, first_row):
    owners = [target_ref[0, first_row + l] // (4 * PAR_DEV) for l in range(LEAF_DEV)]
    ranks = []
    for l in range(LEAF_DEV):
        rank = jnp.int32(0)
        for m in range(l):
            rank = rank + (owners[m] == owners[l]).astype(jnp.int32)
        ranks.append(rank)
    return owners, ranks


def chosen_leaf(owners, ranks, owner, rank):
    chosen = jnp.int32(0)
    for l in range(LEAF_DEV):
        chosen = jnp.where((owners[l] == owner) & (ranks[l] == rank), l, chosen)
    return chosen


def solve_slots(slots, strips, steps, target_ref, front_ref, factor_refs, matrices, store):
    own = lax.axis_index("gy")
    owners, ranks = owner_and_rank(target_ref, own * LEAF_DEV)
    inv_high, inv_low, low_high, low_low = matrices
    leaves = [chosen_leaf(owners, ranks, own ^ k, r) for k, r in slots]
    for i, leaf in enumerate(leaves):
        assemble(steps, factor_refs, (leaf, 0, leaf, i), inv_high, inv_low)
        assemble(steps, factor_refs, (LEAF_DEV + leaf, 1, leaf, i), low_high, low_low)
    for i, leaf in enumerate(leaves):
        sol = product(inv_high[i], inv_low[i], strip_rows(front_ref, leaf * PIV, PIV, strips))
        store(i, leaf, sol, product(low_high[i], low_low[i], sol))


def sent_kernel(steps, slots, capacity, strips, target_ref, front_ref, *refs):
    factor_refs, refs = refs[: len(steps) + 2], refs[len(steps) + 2 :]
    sol_ref, slot_refs, matrices = refs[0], refs[1:-4], refs[-4:]

    def store(i, leaf, sol, update):
        sol_ref[i] = sol
        slot_refs[i // capacity][i % capacity] = update

    solve_slots(slots, strips, steps, target_ref, front_ref, factor_refs, matrices, store)


def kept_kernel(steps, sent, slots, strips, target_ref, front_ref, sent_sol_ref, *refs):
    factor_refs, refs = refs[: len(steps) + 2], refs[len(steps) + 2 :]
    sol_ref, slot_ref, *matrices = refs
    own = lax.axis_index("gy")
    owners, ranks = owner_and_rank(target_ref, own * LEAF_DEV)

    def rows_of(leaf):
        return pl.ds(pl.multiple_of(leaf * PIV, PIV), PIV)

    def store(i, leaf, sol, update):
        sol_ref[rows_of(leaf), :] = sol
        slot_ref[i] = update

    solve_slots(slots, strips, steps, target_ref, front_ref, factor_refs, matrices, store)
    for i, (k, r) in enumerate(sent):
        sol_ref[rows_of(chosen_leaf(owners, ranks, own ^ k, r)), :] = sent_sol_ref[i]


def solve_sent(target, front, factors, slots, capacity, strips):
    steps, blocks = unzip(factors)
    columns = strips * LANES
    shape = functools.partial(jax.ShapeDtypeStruct, dtype=jnp.float32)
    sends = len(slots) // capacity
    out = call(
        functools.partial(sent_kernel, steps, slots, capacity, strips),
        30_000_000,
        16,
        [shape((len(slots), PIV, columns))] + [shape((capacity, 2 * BLK, columns))] * sends,
        [SMEM] + [VMEM] * (1 + len(blocks)),
        [VMEM] * (1 + sends),
        [pltpu.VMEM((len(slots), PIV, PIV), jnp.bfloat16)] * 4,
    )(target, front, *blocks)
    return out[0], out[1:]


def solve_kept(target, front, sent_sol, factors, sent, slots, strips):
    steps, blocks = unzip(factors)
    columns = strips * LANES
    shape = functools.partial(jax.ShapeDtypeStruct, dtype=jnp.float32)
    return call(
        functools.partial(kept_kernel, steps, sent, slots, strips),
        30_000_000,
        16,
        [shape((LEAF_ROWS, columns)), shape((len(slots), 2 * BLK, columns))],
        [SMEM] + [VMEM] * (2 + len(blocks)),
        [VMEM, VMEM],
        [pltpu.VMEM((len(slots), PIV, PIV), jnp.bfloat16)] * 4,
    )(target, front, sent_sol, *blocks)


def subtract_updates(target_ref, relative, slot_ref, reduced):
    own = lax.axis_index("gy")
    first_row = (own ^ relative) * LEAF_DEV
    owners, ranks = owner_and_rank(target_ref, first_row)
    for l in range(LEAF_DEV):

        @pl.when(owners[l] == own)
        def _():
            for j in range(2):
                block = target_ref[j, first_row + l] % OWN_BLOCKS
                at = pl.ds(pl.multiple_of(block * BLK, BLK), BLK)
                reduced[at, :] = reduced[at, :] - slot_ref[ranks[l], pl.ds(j * BLK, BLK), :]


def assemble_kernel(steps, *refs):
    half = PAR_DEV // 2
    for p in range(PAR_DEV):
        assemble(steps, refs[:-2], (p, p // half, p % half, p), *refs[-2:])


def assemble_parents(factors):
    steps, blocks = unzip(factors)
    matrix = jax.ShapeDtypeStruct((PAR_DEV, 4 * BLK, 4 * BLK), jnp.bfloat16)
    return call(
        functools.partial(assemble_kernel, steps), 10_000_000, 8, [matrix, matrix], [VMEM] * len(blocks), [VMEM, VMEM]
    )(*blocks)


def parent_kernel(groups, strips, target_ref, sol_ref, front_ref, high_ref, low_ref, *refs):
    slot_refs, (out_ref, reduced, value, sems) = refs[:groups], refs[groups:]
    leaf_copy = pltpu.make_async_copy(sol_ref, out_ref.at[pl.ds(0, LEAF_ROWS)], sems.at[0])
    leaf_copy.start()
    reduced[...] = strip_rows(front_ref, LEAF_ROWS, PAR_ROWS, strips)
    for k, slot_ref in enumerate(slot_refs):
        subtract_updates(target_ref, k, slot_ref, reduced)
    size = 4 * BLK
    copies = [leaf_copy]
    for p in range(PAR_DEV):
        value[p] = product(high_ref[p], low_ref[p], reduced[pl.ds(p * size, size), :])
        to = out_ref.at[pl.ds(LEAF_ROWS + p * size, size)]
        copies.append(pltpu.make_async_copy(value.at[p], to, sems.at[1 + p]))
        copies[-1].start()
    for copy in copies:
        copy.wait()


def solve_parents(target, sol, front, matrices, slots, strips):
    columns = strips * LANES
    return call(
        functools.partial(parent_kernel, len(slots), strips),
        30_000_000,
        12,
        jax.ShapeDtypeStruct((LEAF_ROWS + PAR_ROWS, columns), jnp.float32),
        [SMEM] + [VMEM] * (4 + len(slots)),
        pl.BlockSpec(memory_space=pl.ANY),
        [
            pltpu.VMEM((PAR_ROWS, columns), jnp.float32),
            pltpu.VMEM((PAR_DEV, 4 * BLK, columns), jnp.float32),
            pltpu.SemaphoreType.DMA((1 + PAR_DEV,)),
        ],
    )(target, sol, front, *matrices, *slots)


def body(right_side, send_order, recv_order, update_target, leaf_inv, leaf_low, parent_inv):
    both = ("gx", "gy")
    n = lax.axis_size(both)
    groups = lax.axis_size("gy")
    rows, columns = right_side.shape
    count = rows // n
    strips = columns // LANES
    capacity = (LEAF_DEV + groups - 1) // groups
    target = update_target.T

    tiles = to_tiles(right_side)
    send, recv = tile_address(send_order, strips), tile_address(recv_order, strips)
    leaf_pieces = ring_gather(side_by_side(leaf_inv, leaf_low), "gz")
    parent_pieces = ring_gather(parent_inv, "gz")

    if n <= 8:
        arrived = [None] * n
        far = [k for k in range(n) if k % groups]
        near = [k for k in range(n) if k % groups == 0]
        packed = {}
        for kinds in [[k] for k in far] + [near]:
            packed.update(zip(kinds, pack(send, tiles, kinds, count, strips)))
        for k in range(n):
            arrived[k] = lax.ppermute(packed[k], both, [(e, e ^ k) for e in range(n)]) if k else packed[0]
    else:
        outgoing = jnp.take(right_side, send_order[0], axis=0, mode="clip")
        arrived = [to_tiles(lax.all_to_all(outgoing, both, split_axis=0, concat_axis=0, tiled=True))]

    relatives = list(range(1, groups))
    sent = [(k, r) for k in relatives for r in range(capacity)]
    kept = [(0, r) for r in range(capacity)]
    front = order_rows(recv, arrived, strips)
    sent_sol, outgoing = solve_sent(target, front, leaf_pieces, sent, capacity, strips)
    slots = []
    for k, slot in zip(relatives, outgoing):
        slots.append(lax.ppermute(slot, "gy", [(g, g ^ k) for g in range(groups)]))
    sol, kept_slot = solve_kept(target, front, sent_sol, leaf_pieces, sent, kept, strips)
    matrices = assemble_parents(parent_pieces)
    return solve_parents(target, sol, front, matrices, [kept_slot] + slots, strips)


def solution(mesh):
    placed = (
        P(("gx", "gy"), "gz"),
        P(("gx", "gy"), None),
        P(("gx", "gy"), None),
        P("gx", None),
        P(("gx", "gy"), "gz", None),
        P(("gx", "gy"), "gz", None),
        P(("gx", "gy"), "gz", None),
    )

    return jax.shard_map(body, mesh=mesh, in_specs=placed, out_specs=P(("gx", "gy"), "gz"), check_vma=False)
```

```python
import functools

import jax
import jax.numpy as jnp
from jax import lax
from jax.experimental import pallas as pl
from jax.experimental.pallas import tpu as pltpu
from jax.sharding import PartitionSpec as P


PIV = 256
BLK = 128
LEAF_DEV = 4
PAR_DEV = 2
LANES = 128
SUBLANES = 8
OWN_BLOCKS = PAR_DEV * 4
LEAF_ROWS = LEAF_DEV * PIV
PAR_ROWS = PAR_DEV * 4 * BLK


SMEM = pl.BlockSpec(memory_space=pltpu.SMEM)
VMEM = pl.BlockSpec(memory_space=pltpu.VMEM)


def call(kernel, flops, grant, out_shape, in_specs, out_specs, scratch_shapes=()):
    return pl.pallas_call(
        kernel,
        out_shape=out_shape,
        in_specs=in_specs,
        out_specs=out_specs,
        scratch_shapes=scratch_shapes,
        cost_estimate=pl.CostEstimate(flops=flops, bytes_accessed=2 << 20, transcendentals=0),
        compiler_params=pltpu.CompilerParams(vmem_limit_bytes=int(grant * (1 << 20))),
    )


def split(value):
    high = value.astype(jnp.bfloat16)
    low = (value - high.astype(jnp.float32)).astype(jnp.bfloat16)
    return high, low


def product(a_high, a_low, b):
    b_high, b_low = split(b)
    dot = functools.partial(jnp.dot, preferred_element_type=jnp.float32)
    return dot(a_high, b_high) + (dot(a_high, b_low) + dot(a_low, b_high))


def to_tiles(rows):
    r, c = rows.shape
    tiles = rows.reshape(r // SUBLANES, SUBLANES, c // LANES, LANES).transpose(0, 2, 1, 3)
    return tiles.reshape(r * (c // LANES), LANES)


def tile_address(row, strips):
    return row * strips - (row & (SUBLANES - 1)) * (strips - 1)


def copy_rows(address_ref, start, source, target, count, strips, unroll=16):
    def step(j, carry):
        base = pl.multiple_of(j * unroll, unroll)
        for u in range(unroll):
            value = source[pl.ds(address_ref[0, start + base + u], strips, stride=SUBLANES), :]
            to = (u // SUBLANES) * SUBLANES * strips + u % SUBLANES
            target[pl.ds(base * strips + to, strips, stride=SUBLANES), :] = value
        return carry

    lax.fori_loop(0, count // unroll, step, 0)


def index_of(axes):
    index = jnp.int32(0)
    for axis in axes:
        index = index * lax.axis_size(axis) + lax.axis_index(axis)
    return index


def pack_kernel(relatives, count, strips, address_ref, rows_ref, *out_refs):
    own = index_of(("gx", "gy"))
    for relative, out_ref in zip(relatives, out_refs):
        copy_rows(address_ref, (own ^ relative) * count, rows_ref, out_ref, count, strips)


def pack(address, tiles, relatives, count, strips):
    shape = jax.ShapeDtypeStruct((count * strips, LANES), jnp.float32)
    return call(
        functools.partial(pack_kernel, relatives, count, strips),
        10_000_000,
        8,
        [shape] * len(relatives),
        [SMEM, VMEM],
        [VMEM] * len(relatives),
    )(address, tiles)


def stack_arrived(piece_refs, arrived):
    own = index_of(("gx", "gy"))
    each = piece_refs[0].shape[0]
    for k, ref in enumerate(piece_refs):
        at = (own ^ k) * each if len(piece_refs) > 1 else 0
        arrived[pl.ds(pl.multiple_of(at, SUBLANES), each), :] = ref[...]


def strip_rows(ref, first, rows, strips):
    at = pl.ds(pl.multiple_of(first * strips, SUBLANES), rows * strips)
    tiles = ref[at, :].reshape(rows // SUBLANES, strips, SUBLANES, LANES)
    return jnp.concatenate([tiles[:, s].reshape(rows, LANES) for s in range(strips)], axis=1)


def order_kernel(pieces, strips, address_ref, *refs):
    piece_refs, front_ref, arrived = refs[:pieces], *refs[pieces:]
    stack_arrived(piece_refs, arrived)
    copy_rows(address_ref, 0, arrived, front_ref, arrived.shape[0] // strips, strips)


def order_rows(address, pieces, strips):
    shape = (sum(piece.shape[0] for piece in pieces), LANES)
    return call(
        functools.partial(order_kernel, len(pieces), strips),
        10_000_000,
        12,
        jax.ShapeDtypeStruct(shape, jnp.float32),
        [SMEM] + [VMEM] * len(pieces),
        VMEM,
        [pltpu.VMEM(shape, jnp.float32)],
    )(address, *pieces)


def side_by_side(a, b):
    least = jnp.float32(-jnp.inf)
    rest = [(0, 0, 0)] * (a.ndim - 1)
    return jnp.maximum(
        lax.pad(a, least, [(0, b.shape[0], 0)] + rest), lax.pad(b, least, [(a.shape[0], 0, 0)] + rest)
    )


def ring_order(n):
    return list(range(0, n, 2)) + list(range(n - 1, 0, -2))


def ring_gather(block, axis):
    n = lax.axis_size(axis)
    assert n % 2 == 0
    ring = ring_order(n)
    forward = [(ring[i], ring[(i + 1) % n]) for i in range(n)]
    backward = [(b, a) for a, b in forward]

    def hop(value, way):
        return lax.ppermute(value, axis, forward if way == "f" else backward)

    pieces = [(0, block)]
    ahead = behind = block
    for step in range(1, n // 2):
        ahead, behind = hop(ahead, "f"), hop(behind, "b")
        pieces += [(step, ahead), (-step, behind)]
    half = block.shape[0] // 2
    return pieces, (hop(ahead[:half], "f"), hop(behind[half:], "b"))


def unzip(factors):
    pieces, halves = factors
    return [step for step, _ in pieces], [block for _, block in pieces] + list(halves)


def place_of(steps):
    n = lax.axis_size("gz")
    index = lax.axis_index("gz")
    at = jnp.where(index % 2 == 0, index // 2, n - 1 - index // 2)
    to = (at - steps + n) % n
    return jnp.where(to < n // 2, 2 * to, 2 * (n - to) - 1)


def assemble(steps, refs, entry, high, low):
    at_piece, half, at_half, slot = entry
    parts = [(step, ref, at_piece) for step, ref in zip(steps, refs)]
    parts.append((lax.axis_size("gz") // 2, refs[len(steps) + half], at_half))
    for step, ref, index in parts:
        rows = ref.shape[1]
        at = pl.ds(pl.multiple_of(place_of(step) * rows, rows), rows)
        high[slot, at, :], low[slot, at, :] = split(ref[index])


def owner_and_rank(target_ref, first_row):
    owners = [target_ref[0, first_row + l] // (4 * PAR_DEV) for l in range(LEAF_DEV)]
    ranks = []
    for l in range(LEAF_DEV):
        rank = jnp.int32(0)
        for m in range(l):
            rank = rank + (owners[m] == owners[l]).astype(jnp.int32)
        ranks.append(rank)
    return owners, ranks


def chosen_leaf(owners, ranks, owner, rank):
    chosen = jnp.int32(0)
    for l in range(LEAF_DEV):
        chosen = jnp.where((owners[l] == owner) & (ranks[l] == rank), l, chosen)
    return chosen


def solve_slots(slots, strips, steps, target_ref, front_ref, factor_refs, matrices, store):
    own = lax.axis_index("gy")
    owners, ranks = owner_and_rank(target_ref, own * LEAF_DEV)
    inv_high, inv_low, low_high, low_low = matrices
    leaves = [chosen_leaf(owners, ranks, own ^ k, r) for k, r in slots]
    for i, leaf in enumerate(leaves):
        assemble(steps, factor_refs, (leaf, 0, leaf, i), inv_high, inv_low)
        assemble(steps, factor_refs, (LEAF_DEV + leaf, 1, leaf, i), low_high, low_low)
    for i, leaf in enumerate(leaves):
        sol = product(inv_high[i], inv_low[i], strip_rows(front_ref, leaf * PIV, PIV, strips))
        store(i, leaf, sol, product(low_high[i], low_low[i], sol))


def sent_kernel(steps, slots, capacity, strips, target_ref, front_ref, *refs):
    factor_refs, refs = refs[: len(steps) + 2], refs[len(steps) + 2 :]
    sol_ref, slot_refs, matrices = refs[0], refs[1:-4], refs[-4:]

    def store(i, leaf, sol, update):
        sol_ref[i] = sol
        slot_refs[i // capacity][i % capacity] = update

    solve_slots(slots, strips, steps, target_ref, front_ref, factor_refs, matrices, store)


def kept_kernel(steps, sent, slots, strips, target_ref, front_ref, sent_sol_ref, *refs):
    factor_refs, refs = refs[: len(steps) + 2], refs[len(steps) + 2 :]
    sol_ref, slot_ref, *matrices = refs
    own = lax.axis_index("gy")
    owners, ranks = owner_and_rank(target_ref, own * LEAF_DEV)

    def rows_of(leaf):
        return pl.ds(pl.multiple_of(leaf * PIV, PIV), PIV)

    def store(i, leaf, sol, update):
        sol_ref[rows_of(leaf), :] = sol
        slot_ref[i] = update

    solve_slots(slots, strips, steps, target_ref, front_ref, factor_refs, matrices, store)
    for i, (k, r) in enumerate(sent):
        sol_ref[rows_of(chosen_leaf(owners, ranks, own ^ k, r)), :] = sent_sol_ref[i]


def solve_sent(target, front, factors, slots, capacity, strips):
    steps, blocks = unzip(factors)
    columns = strips * LANES
    shape = functools.partial(jax.ShapeDtypeStruct, dtype=jnp.float32)
    sends = len(slots) // capacity
    out = call(
        functools.partial(sent_kernel, steps, slots, capacity, strips),
        30_000_000,
        16,
        [shape((len(slots), PIV, columns))] + [shape((capacity, 2 * BLK, columns))] * sends,
        [SMEM] + [VMEM] * (1 + len(blocks)),
        [VMEM] * (1 + sends),
        [pltpu.VMEM((len(slots), PIV, PIV), jnp.bfloat16)] * 4,
    )(target, front, *blocks)
    return out[0], out[1:]


def solve_kept(target, front, sent_sol, factors, sent, slots, strips):
    steps, blocks = unzip(factors)
    columns = strips * LANES
    shape = functools.partial(jax.ShapeDtypeStruct, dtype=jnp.float32)
    return call(
        functools.partial(kept_kernel, steps, sent, slots, strips),
        30_000_000,
        16,
        [shape((LEAF_ROWS, columns)), shape((len(slots), 2 * BLK, columns))],
        [SMEM] + [VMEM] * (2 + len(blocks)),
        [VMEM, VMEM],
        [pltpu.VMEM((len(slots), PIV, PIV), jnp.bfloat16)] * 4,
    )(target, front, sent_sol, *blocks)


def joining(target_ref, relative, rank):
    own = lax.axis_index("gy")
    first_row = (own ^ relative) * LEAF_DEV
    owners, ranks = owner_and_rank(target_ref, first_row)
    present = jnp.bool_(False)
    for l in range(LEAF_DEV):
        present = present | ((owners[l] == own) & (ranks[l] == rank))
    row = first_row + chosen_leaf(owners, ranks, own, rank)
    return present, [target_ref[j, row] % OWN_BLOCKS for j in range(2)]


def base_kernel(steps, capacity, strips, target_ref, front_ref, slot_ref, *refs):
    factor_refs, (high, low, base, reduced) = refs[: len(steps) + 2], refs[len(steps) + 2 :]
    half = PAR_DEV // 2
    for p in range(PAR_DEV):
        assemble(steps, factor_refs, (p, p // half, p % half, p), high, low)
    reduced[...] = strip_rows(front_ref, LEAF_ROWS, PAR_ROWS, strips)
    for r in range(capacity):
        present, blocks = joining(target_ref, 0, r)

        @pl.when(present)
        def _():
            for j, block in enumerate(blocks):
                at = pl.ds(pl.multiple_of(block * BLK, BLK), BLK)
                reduced[at, :] = reduced[at, :] - slot_ref[r, pl.ds(j * BLK, BLK), :]

    size = 4 * BLK
    for p in range(PAR_DEV):
        base[p] = product(high[p], low[p], reduced[pl.ds(p * size, size), :])


def base_parents(target, front, slot, factors, capacity, strips):
    steps, blocks = unzip(factors)
    size, columns = 4 * BLK, strips * LANES
    matrix = jax.ShapeDtypeStruct((PAR_DEV, size, size), jnp.bfloat16)
    return call(
        functools.partial(base_kernel, steps, capacity, strips),
        30_000_000,
        12,
        [matrix, matrix, jax.ShapeDtypeStruct((PAR_DEV, size, columns), jnp.float32)],
        [SMEM] + [VMEM] * (2 + len(blocks)),
        [VMEM] * 3,
        [pltpu.VMEM((PAR_ROWS, columns), jnp.float32)],
    )(target, front, slot, *blocks)


def parent_kernel(relatives, capacity, target_ref, sol_ref, high_ref, low_ref, base_ref, *refs):
    slot_refs, (out_ref, value, sems) = refs[: len(relatives)], refs[len(relatives) :]
    copies = [pltpu.make_async_copy(sol_ref, out_ref.at[pl.ds(0, LEAF_ROWS)], sems.at[0])]
    copies[0].start()
    value[...] = base_ref[...]
    for k, slot_ref in zip(relatives, slot_refs):
        for r in range(capacity):
            present, blocks = joining(target_ref, k, r)
            p = blocks[0] // 4
            lanes = [pl.ds(pl.multiple_of((block % 4) * BLK, BLK), BLK) for block in blocks]

            @pl.when(present)
            def _():
                high, low = [jnp.concatenate([ref[p, :, at] for at in lanes], axis=1) for ref in (high_ref, low_ref)]
                value[p] = value[p] - product(high, low, slot_ref[r])

    for p in range(PAR_DEV):
        to = out_ref.at[pl.ds(LEAF_ROWS + p * 4 * BLK, 4 * BLK)]
        copies.append(pltpu.make_async_copy(value.at[p], to, sems.at[1 + p]))
        copies[-1].start()
    for copy in copies:
        copy.wait()


def solve_parents(target, sol, parts, relatives, slots, capacity):
    return call(
        functools.partial(parent_kernel, relatives, capacity),
        30_000_000,
        12,
        jax.ShapeDtypeStruct((LEAF_ROWS + PAR_ROWS, sol.shape[1]), jnp.float32),
        [SMEM] + [VMEM] * (4 + len(slots)),
        pl.BlockSpec(memory_space=pl.ANY),
        [
            pltpu.VMEM((PAR_DEV, 4 * BLK, sol.shape[1]), jnp.float32),
            pltpu.SemaphoreType.DMA((1 + PAR_DEV,)),
        ],
    )(target, sol, *parts, *slots)


def body(right_side, send_order, recv_order, update_target, leaf_inv, leaf_low, parent_inv):
    both = ("gx", "gy")
    n = lax.axis_size(both)
    groups = lax.axis_size("gy")
    rows, columns = right_side.shape
    count = rows // n
    strips = columns // LANES
    capacity = (LEAF_DEV + groups - 1) // groups
    target = update_target.T

    tiles = to_tiles(right_side)
    send, recv = tile_address(send_order, strips), tile_address(recv_order, strips)
    leaf_pieces = ring_gather(side_by_side(leaf_inv, leaf_low), "gz")
    parent_pieces = ring_gather(parent_inv, "gz")

    if n <= 8:
        arrived = [None] * n
        far = [k for k in range(n) if k % groups]
        near = [k for k in range(n) if k % groups == 0]
        packed = {}
        for kinds in [[k] for k in far] + [near]:
            packed.update(zip(kinds, pack(send, tiles, kinds, count, strips)))
        for k in range(n):
            arrived[k] = lax.ppermute(packed[k], both, [(e, e ^ k) for e in range(n)]) if k else packed[0]
    else:
        outgoing = jnp.take(right_side, send_order[0], axis=0, mode="clip")
        arrived = [to_tiles(lax.all_to_all(outgoing, both, split_axis=0, concat_axis=0, tiled=True))]

    relatives = list(range(1, groups))
    sent = [(k, r) for k in relatives for r in range(capacity)]
    kept = [(0, r) for r in range(capacity)]
    front = order_rows(recv, arrived, strips)
    sent_sol, outgoing = solve_sent(target, front, leaf_pieces, sent, capacity, strips)
    slots = []
    for k, slot in zip(relatives, outgoing):
        slots.append(lax.ppermute(slot, "gy", [(g, g ^ k) for g in range(groups)]))
    sol, kept_slot = solve_kept(target, front, sent_sol, leaf_pieces, sent, kept, strips)
    parts = base_parents(target, front, kept_slot, parent_pieces, capacity, strips)
    return solve_parents(target, sol, parts, relatives, slots, capacity)


def solution(mesh):
    placed = (
        P(("gx", "gy"), "gz"),
        P(("gx", "gy"), None),
        P(("gx", "gy"), None),
        P("gx", None),
        P(("gx", "gy"), "gz", None),
        P(("gx", "gy"), "gz", None),
        P(("gx", "gy"), "gz", None),
    )

    return jax.shard_map(body, mesh=mesh, in_specs=placed, out_specs=P(("gx", "gy"), "gz"), check_vma=False)
```

```python
import functools

import jax
import jax.numpy as jnp
from jax import lax
from jax.experimental import pallas as pl
from jax.experimental.pallas import tpu as pltpu
from jax.sharding import PartitionSpec as P


PIV = 256
BLK = 128
LEAF_DEV = 4
PAR_DEV = 2
LANES = 128
SUBLANES = 8
OWN_BLOCKS = PAR_DEV * 4
LEAF_ROWS = LEAF_DEV * PIV
PAR_ROWS = PAR_DEV * 4 * BLK


SMEM = pl.BlockSpec(memory_space=pltpu.SMEM)
VMEM = pl.BlockSpec(memory_space=pltpu.VMEM)


def call(kernel, flops, grant, out_shape, in_specs, out_specs, scratch_shapes=()):
    return pl.pallas_call(
        kernel,
        out_shape=out_shape,
        in_specs=in_specs,
        out_specs=out_specs,
        scratch_shapes=scratch_shapes,
        cost_estimate=pl.CostEstimate(flops=flops, bytes_accessed=2 << 20, transcendentals=0),
        compiler_params=pltpu.CompilerParams(vmem_limit_bytes=int(grant * (1 << 20))),
    )


def split(value):
    high = value.astype(jnp.bfloat16)
    low = (value - high.astype(jnp.float32)).astype(jnp.bfloat16)
    return high, low


def product(a_high, a_low, b):
    b_high, b_low = split(b)
    dot = functools.partial(jnp.dot, preferred_element_type=jnp.float32)
    return dot(a_high, b_high) + (dot(a_high, b_low) + dot(a_low, b_high))


def to_tiles(rows):
    r, c = rows.shape
    tiles = rows.reshape(r // SUBLANES, SUBLANES, c // LANES, LANES).transpose(0, 2, 1, 3)
    return tiles.reshape(r * (c // LANES), LANES)


def tile_address(row, strips):
    return row * strips - (row & (SUBLANES - 1)) * (strips - 1)


def copy_rows(address_ref, start, source, target, count, strips, unroll=128):
    def step(j, carry):
        base = pl.multiple_of(j * unroll, unroll)
        for u in range(unroll):
            value = source[pl.ds(address_ref[0, start + base + u], strips, stride=SUBLANES), :]
            to = (u // SUBLANES) * SUBLANES * strips + u % SUBLANES
            target[pl.ds(base * strips + to, strips, stride=SUBLANES), :] = value
        return carry

    lax.fori_loop(0, count // unroll, step, 0)


def index_of(axes):
    index = jnp.int32(0)
    for axis in axes:
        index = index * lax.axis_size(axis) + lax.axis_index(axis)
    return index


def pack_kernel(relatives, count, strips, address_ref, rows_ref, *out_refs):
    own = index_of(("gx", "gy"))
    for relative, out_ref in zip(relatives, out_refs):
        copy_rows(address_ref, (own ^ relative) * count, rows_ref, out_ref, count, strips)


def pack(address, tiles, relatives, count, strips):
    shape = jax.ShapeDtypeStruct((count * strips, LANES), jnp.float32)
    return call(
        functools.partial(pack_kernel, relatives, count, strips),
        10_000_000,
        8,
        [shape] * len(relatives),
        [SMEM, VMEM],
        [VMEM] * len(relatives),
    )(address, tiles)


def stack_arrived(piece_refs, arrived):
    own = index_of(("gx", "gy"))
    each = piece_refs[0].shape[0]
    for k, ref in enumerate(piece_refs):
        at = (own ^ k) * each if len(piece_refs) > 1 else 0
        arrived[pl.ds(pl.multiple_of(at, SUBLANES), each), :] = ref[...]


def strip_rows(ref, first, rows, strips):
    at = pl.ds(pl.multiple_of(first * strips, SUBLANES), rows * strips)
    tiles = ref[at, :].reshape(rows // SUBLANES, strips, SUBLANES, LANES)
    return jnp.concatenate([tiles[:, s].reshape(rows, LANES) for s in range(strips)], axis=1)


def order_kernel(pieces, strips, address_ref, *refs):
    piece_refs, front_ref, arrived_ref = refs[:pieces], *refs[pieces:]
    stack_arrived(piece_refs, arrived_ref)
    copy_rows(address_ref, 0, arrived_ref, front_ref, front_ref.shape[0] // strips, strips)


def order_leaves(address, pieces, strips):
    arrived = jax.ShapeDtypeStruct((sum(piece.shape[0] for piece in pieces), LANES), jnp.float32)
    return call(
        functools.partial(order_kernel, len(pieces), strips),
        10_000_000,
        12,
        [jax.ShapeDtypeStruct((LEAF_ROWS * strips, LANES), jnp.float32), arrived],
        [SMEM] + [VMEM] * len(pieces),
        [VMEM, VMEM],
    )(address, *pieces)


def rest_kernel(strips, address_ref, arrived_ref, front_ref):
    copy_rows(address_ref, LEAF_ROWS, arrived_ref, front_ref, PAR_ROWS, strips)


def order_parents(address, arrived, strips):
    return call(
        functools.partial(rest_kernel, strips),
        10_000_000,
        8,
        jax.ShapeDtypeStruct((PAR_ROWS * strips, LANES), jnp.float32),
        [SMEM, VMEM],
        VMEM,
    )(address, arrived)


def side_by_side(a, b):
    least = jnp.float32(-jnp.inf)
    rest = [(0, 0, 0)] * (a.ndim - 1)
    return jnp.maximum(
        lax.pad(a, least, [(0, b.shape[0], 0)] + rest), lax.pad(b, least, [(a.shape[0], 0, 0)] + rest)
    )


def ring_order(n):
    return list(range(0, n, 2)) + list(range(n - 1, 0, -2))


def ring_gather(block, axis):
    n = lax.axis_size(axis)
    assert n % 2 == 0
    ring = ring_order(n)
    forward = [(ring[i], ring[(i + 1) % n]) for i in range(n)]
    backward = [(b, a) for a, b in forward]

    def hop(value, way):
        return lax.ppermute(value, axis, forward if way == "f" else backward)

    pieces = [(0, block)]
    ahead = behind = block
    for step in range(1, n // 2):
        ahead, behind = hop(ahead, "f"), hop(behind, "b")
        pieces += [(step, ahead), (-step, behind)]
    half = block.shape[0] // 2
    return pieces, (hop(ahead[:half], "f"), hop(behind[half:], "b"))


def unzip(factors):
    pieces, halves = factors
    return [step for step, _ in pieces], [block for _, block in pieces] + list(halves)


def place_of(steps):
    n = lax.axis_size("gz")
    index = lax.axis_index("gz")
    at = jnp.where(index % 2 == 0, index // 2, n - 1 - index // 2)
    to = (at - steps + n) % n
    return jnp.where(to < n // 2, 2 * to, 2 * (n - to) - 1)


def assemble(steps, refs, entry, high, low):
    at_piece, half, at_half, slot = entry
    parts = [(step, ref, at_piece) for step, ref in zip(steps, refs)]
    parts.append((lax.axis_size("gz") // 2, refs[len(steps) + half], at_half))
    for step, ref, index in parts:
        rows = ref.shape[1]
        at = pl.ds(pl.multiple_of(place_of(step) * rows, rows), rows)
        high[slot, at, :], low[slot, at, :] = split(ref[index])


def owner_and_rank(target_ref, first_row):
    owners = [target_ref[0, first_row + l] // (4 * PAR_DEV) for l in range(LEAF_DEV)]
    ranks = []
    for l in range(LEAF_DEV):
        rank = jnp.int32(0)
        for m in range(l):
            rank = rank + (owners[m] == owners[l]).astype(jnp.int32)
        ranks.append(rank)
    return owners, ranks


def chosen_leaf(owners, ranks, owner, rank):
    chosen = jnp.int32(0)
    for l in range(LEAF_DEV):
        chosen = jnp.where((owners[l] == owner) & (ranks[l] == rank), l, chosen)
    return chosen


def solve_slots(slots, strips, steps, target_ref, front_ref, factor_refs, matrices, store):
    own = lax.axis_index("gy")
    owners, ranks = owner_and_rank(target_ref, own * LEAF_DEV)
    inv_high, inv_low, low_high, low_low = matrices
    leaves = [chosen_leaf(owners, ranks, own ^ k, r) for k, r in slots]
    for i, leaf in enumerate(leaves):
        assemble(steps, factor_refs, (leaf, 0, leaf, i), inv_high, inv_low)
        assemble(steps, factor_refs, (LEAF_DEV + leaf, 1, leaf, i), low_high, low_low)
    for i, leaf in enumerate(leaves):
        sol = product(inv_high[i], inv_low[i], strip_rows(front_ref, leaf * PIV, PIV, strips))
        store(i, leaf, sol, product(low_high[i], low_low[i], sol))


def sent_kernel(steps, slots, capacity, strips, target_ref, front_ref, *refs):
    factor_refs, refs = refs[: len(steps) + 2], refs[len(steps) + 2 :]
    sol_ref, slot_refs, matrices = refs[0], refs[1:-4], refs[-4:]

    def store(i, leaf, sol, update):
        sol_ref[i] = sol
        slot_refs[i // capacity][i % capacity] = update

    solve_slots(slots, strips, steps, target_ref, front_ref, factor_refs, matrices, store)


def kept_kernel(steps, sent, slots, strips, target_ref, front_ref, sent_sol_ref, *refs):
    factor_refs, refs = refs[: len(steps) + 2], refs[len(steps) + 2 :]
    sol_ref, slot_ref, *matrices = refs
    own = lax.axis_index("gy")
    owners, ranks = owner_and_rank(target_ref, own * LEAF_DEV)

    def rows_of(leaf):
        return pl.ds(pl.multiple_of(leaf * PIV, PIV), PIV)

    def store(i, leaf, sol, update):
        sol_ref[rows_of(leaf), :] = sol
        slot_ref[i] = update

    solve_slots(slots, strips, steps, target_ref, front_ref, factor_refs, matrices, store)
    for i, (k, r) in enumerate(sent):
        sol_ref[rows_of(chosen_leaf(owners, ranks, own ^ k, r)), :] = sent_sol_ref[i]


def solve_sent(target, front, factors, slots, capacity, strips):
    steps, blocks = unzip(factors)
    columns = strips * LANES
    shape = functools.partial(jax.ShapeDtypeStruct, dtype=jnp.float32)
    sends = len(slots) // capacity
    out = call(
        functools.partial(sent_kernel, steps, slots, capacity, strips),
        30_000_000,
        16,
        [shape((len(slots), PIV, columns))] + [shape((capacity, 2 * BLK, columns))] * sends,
        [SMEM] + [VMEM] * (1 + len(blocks)),
        [VMEM] * (1 + sends),
        [pltpu.VMEM((len(slots), PIV, PIV), jnp.bfloat16)] * 4,
    )(target, front, *blocks)
    return out[0], out[1:]


def solve_kept(target, front, sent_sol, factors, sent, slots, strips):
    steps, blocks = unzip(factors)
    columns = strips * LANES
    shape = functools.partial(jax.ShapeDtypeStruct, dtype=jnp.float32)
    return call(
        functools.partial(kept_kernel, steps, sent, slots, strips),
        30_000_000,
        16,
        [shape((LEAF_ROWS, columns)), shape((len(slots), 2 * BLK, columns))],
        [SMEM] + [VMEM] * (2 + len(blocks)),
        [VMEM, VMEM],
        [pltpu.VMEM((len(slots), PIV, PIV), jnp.bfloat16)] * 4,
    )(target, front, sent_sol, *blocks)


def joining(target_ref, relative, rank):
    own = lax.axis_index("gy")
    first_row = (own ^ relative) * LEAF_DEV
    owners, ranks = owner_and_rank(target_ref, first_row)
    present = jnp.bool_(False)
    for l in range(LEAF_DEV):
        present = present | ((owners[l] == own) & (ranks[l] == rank))
    row = first_row + chosen_leaf(owners, ranks, own, rank)
    return present, [target_ref[j, row] % OWN_BLOCKS for j in range(2)]


def base_kernel(steps, capacity, strips, target_ref, front_ref, slot_ref, *refs):
    factor_refs, (high, low, base, reduced) = refs[: len(steps) + 2], refs[len(steps) + 2 :]
    half = PAR_DEV // 2
    for p in range(PAR_DEV):
        assemble(steps, factor_refs, (p, p // half, p % half, p), high, low)
    reduced[...] = strip_rows(front_ref, 0, PAR_ROWS, strips)
    for r in range(capacity):
        present, blocks = joining(target_ref, 0, r)

        @pl.when(present)
        def _():
            for j, block in enumerate(blocks):
                at = pl.ds(pl.multiple_of(block * BLK, BLK), BLK)
                reduced[at, :] = reduced[at, :] - slot_ref[r, pl.ds(j * BLK, BLK), :]

    size = 4 * BLK
    for p in range(PAR_DEV):
        base[p] = product(high[p], low[p], reduced[pl.ds(p * size, size), :])


def base_parents(target, front, slot, factors, capacity, strips):
    steps, blocks = unzip(factors)
    size, columns = 4 * BLK, strips * LANES
    matrix = jax.ShapeDtypeStruct((PAR_DEV, size, size), jnp.bfloat16)
    return call(
        functools.partial(base_kernel, steps, capacity, strips),
        30_000_000,
        12,
        [matrix, matrix, jax.ShapeDtypeStruct((PAR_DEV, size, columns), jnp.float32)],
        [SMEM] + [VMEM] * (2 + len(blocks)),
        [VMEM] * 3,
        [pltpu.VMEM((PAR_ROWS, columns), jnp.float32)],
    )(target, front, slot, *blocks)


def parent_kernel(relatives, capacity, target_ref, sol_ref, high_ref, low_ref, base_ref, *refs):
    slot_refs, (out_ref, value, sems) = refs[: len(relatives)], refs[len(relatives) :]
    copies = [pltpu.make_async_copy(sol_ref, out_ref.at[pl.ds(0, LEAF_ROWS)], sems.at[0])]
    copies[0].start()
    value[...] = base_ref[...]
    for k, slot_ref in zip(relatives, slot_refs):
        for r in range(capacity):
            present, blocks = joining(target_ref, k, r)
            p = blocks[0] // 4
            lanes = [pl.ds(pl.multiple_of((block % 4) * BLK, BLK), BLK) for block in blocks]

            @pl.when(present)
            def _():
                high, low = [jnp.concatenate([ref[p, :, at] for at in lanes], axis=1) for ref in (high_ref, low_ref)]
                value[p] = value[p] - product(high, low, slot_ref[r])

    for p in range(PAR_DEV):
        to = out_ref.at[pl.ds(LEAF_ROWS + p * 4 * BLK, 4 * BLK)]
        copies.append(pltpu.make_async_copy(value.at[p], to, sems.at[1 + p]))
        copies[-1].start()
    for copy in copies:
        copy.wait()


def solve_parents(target, sol, parts, relatives, slots, capacity):
    return call(
        functools.partial(parent_kernel, relatives, capacity),
        30_000_000,
        12,
        jax.ShapeDtypeStruct((LEAF_ROWS + PAR_ROWS, sol.shape[1]), jnp.float32),
        [SMEM] + [VMEM] * (4 + len(slots)),
        pl.BlockSpec(memory_space=pl.ANY),
        [
            pltpu.VMEM((PAR_DEV, 4 * BLK, sol.shape[1]), jnp.float32),
            pltpu.SemaphoreType.DMA((1 + PAR_DEV,)),
        ],
    )(target, sol, *parts, *slots)


def body(right_side, send_order, recv_order, update_target, leaf_inv, leaf_low, parent_inv):
    both = ("gx", "gy")
    n = lax.axis_size(both)
    groups = lax.axis_size("gy")
    rows, columns = right_side.shape
    count = rows // n
    strips = columns // LANES
    capacity = (LEAF_DEV + groups - 1) // groups
    target = update_target.T

    tiles = to_tiles(right_side)
    send, recv = tile_address(send_order, strips), tile_address(recv_order, strips)
    leaf_pieces = ring_gather(side_by_side(leaf_inv, leaf_low), "gz")
    parent_pieces = ring_gather(parent_inv, "gz")

    if n <= 8:
        arrived = [None] * n
        far = [k for k in range(n) if k % groups]
        near = [k for k in range(n) if k % groups == 0]
        packed = {}
        for kinds in [[k] for k in far] + [near]:
            packed.update(zip(kinds, pack(send, tiles, kinds, count, strips)))
        for k in range(n):
            arrived[k] = lax.ppermute(packed[k], both, [(e, e ^ k) for e in range(n)]) if k else packed[0]
    else:
        outgoing = jnp.take(right_side, send_order[0], axis=0, mode="clip")
        arrived = [to_tiles(lax.all_to_all(outgoing, both, split_axis=0, concat_axis=0, tiled=True))]

    relatives = list(range(1, groups))
    sent = [(k, r) for k in relatives for r in range(capacity)]
    kept = [(0, r) for r in range(capacity)]
    front, arrived = order_leaves(recv, arrived, strips)
    sent_sol, outgoing = solve_sent(target, front, leaf_pieces, sent, capacity, strips)
    slots = []
    for k, slot in zip(relatives, outgoing):
        slots.append(lax.ppermute(slot, "gy", [(g, g ^ k) for g in range(groups)]))
    sol, kept_slot = solve_kept(target, front, sent_sol, leaf_pieces, sent, kept, strips)
    front = order_parents(recv, arrived, strips)
    parts = base_parents(target, front, kept_slot, parent_pieces, capacity, strips)
    return solve_parents(target, sol, parts, relatives, slots, capacity)


def solution(mesh):
    placed = (
        P(("gx", "gy"), "gz"),
        P(("gx", "gy"), None),
        P(("gx", "gy"), None),
        P("gx", None),
        P(("gx", "gy"), "gz", None),
        P(("gx", "gy"), "gz", None),
        P(("gx", "gy"), "gz", None),
    )

    return jax.shard_map(body, mesh=mesh, in_specs=placed, out_specs=P(("gx", "gy"), "gz"), check_vma=False)
```
